8 devices in a mesh: dp: 2 (over y, z), ep: 4 (over x, core).
Axes of the slice: x: 2, y: 2, z: 1, core: 2. Of those that a mesh axis runs over, the one named last changes fastest.
Arguments:
- x: bfloat16 [2, 4, 512, 4096], P('dp', 'ep'), parts along dimension 0
- expert: int32 [2, 4, 512, 8], P('dp', 'ep'), parts along dimension 0
- slot: int32 [2, 4, 512, 8], P('dp', 'ep'), parts along dimension 0
- gate: float32 [2, 4, 512, 8], P('dp', 'ep'), parts along dimension 0
- w_gate: bfloat16 [64, 4096, 1536], P('ep')
- w_up: bfloat16 [64, 4096, 1536], P('ep')
- w_down: bfloat16 [64, 1536, 4096], P('ep')
Outputs:
- y: bfloat16 [2, 4, 512, 4096], P('dp', 'ep'), parts along dimension 0
There are 2 independent parts. The reference program is written for one: setup_inputs(seed, part) draws one part's arguments, and reference() takes and returns one part's arrays. A program takes and returns all parts, laid end to end along the dimension named above; an argument that names none is the same for every part.
All inputs are finite; a program needn't handle non-finite values.
Results may differ from the reference program's by a relative error of at most 0.009.
Values are sent between devices in bfloat16 or wider.
A program may use at most 2 GiB of HBM per device.

```python
import jax
import jax.numpy as jnp

MEMBERS = 4
TOKENS = 512
D = 4096
FF = 1536
TOP = 8
EXPERTS = 64
SLOTS = 5 * TOKENS * TOP // (4 * EXPERTS)


def setup_inputs(seed: int = 0, part: int = 0) -> dict:
    own, k1, k2, k3, k4, k5, k6 = jax.random.split(jax.random.key(seed), 7)
    kx, ke, kl, kg = jax.random.split(jax.random.fold_in(own, part), 4)
    devices = (1, MEMBERS)
    place = jax.random.permutation(kl, jnp.arange(EXPERTS, dtype=jnp.uint32))
    slow = ((EXPERTS + (9 * place) % EXPERTS) << ((9 * place) // EXPERTS)) // EXPERTS
    wait = (jax.random.bits(ke, (*devices, TOKENS, EXPERTS), jnp.uint32) >> 10) * slow
    expert = jnp.argsort(wait, axis=-1)[..., :TOP].astype(jnp.int32)
    chosen = jax.nn.one_hot(expert, EXPERTS, dtype=jnp.int32)
    in_line = jnp.cumsum(chosen.reshape(*devices, TOKENS * TOP, EXPERTS), axis=2) - 1
    slot = jnp.sum(in_line.reshape(chosen.shape) * chosen, axis=-1)

    def one(key, rows, columns):
        return (jax.random.normal(key, (rows, columns), jnp.float32) * rows**-0.5).astype(jnp.bfloat16)

    def weights(key, rows, columns):
        return jax.lax.map(lambda k: one(k, rows, columns), jax.random.split(key, EXPERTS))

    return {
        "x": jax.random.normal(kx, (*devices, TOKENS, D), jnp.float32).astype(jnp.bfloat16),
        "expert": expert,
        "slot": slot,
        "gate": jax.nn.softmax(jax.random.normal(kg, expert.shape, jnp.float32)),
        "w_gate": weights(k1, D, FF),
        "w_up": weights(k2, D, FF),
        "w_down": weights(k3, FF, D),
    }


def einsum(form, a, b):
    return jnp.einsum(form, a.astype(jnp.float32), b.astype(jnp.float32))


def reference(x, expert, slot, gate, w_gate, w_up, w_down):
    to_expert = jax.nn.one_hot(expert, EXPERTS, dtype=jnp.bfloat16)
    to_slot = jax.nn.one_hot(slot, SLOTS, dtype=jnp.bfloat16)
    weighted = to_expert * gate[..., None].astype(jnp.bfloat16)
    dispatch = einsum("abtke,abtkc->abtec", to_expert, to_slot).astype(jnp.bfloat16)
    combine = einsum("abtke,abtkc->abtec", weighted, to_slot).astype(jnp.bfloat16)
    z = einsum("abtec,abtd->aebcd", dispatch, x).astype(jnp.bfloat16)
    h = jax.nn.silu(einsum("aebcd,edf->aebcf", z, w_gate))
    h = (h * einsum("aebcd,edf->aebcf", z, w_up)).astype(jnp.bfloat16)
    out = einsum("aebcf,efd->aebcd", h, w_down).astype(jnp.bfloat16)
    y = einsum("abtec,aebcd->abtd", combine, out)
    return y.astype(jnp.bfloat16)
```

```python
import jax
import jax.numpy as jnp
from jax import lax
from jax.experimental import pallas as pl
from jax.experimental.pallas import tpu as pltpu
from jax.sharding import PartitionSpec as P

F32, BF16, I32 = jnp.float32, jnp.bfloat16, jnp.int32
VMEM_LIMIT = 64 * 1024 * 1024 - 64 * 1024 * 2
GROUP = 16
CHUNKS = (1024, 1024, 1024, 512, 512)
ANY = pl.BlockSpec(memory_space=pl.ANY)


def params(*semantics):
    return pltpu.CompilerParams(dimension_semantics=semantics, vmem_limit_bytes=VMEM_LIMIT)


def dispatch(rows_used, place, x, rows):
    top, tokens = place.shape
    d = x.shape[1]
    tile = min(d, 1024)
    block = 256

    def kernel(used_ref, place_ref, x_ref, z_ref, hot_ref):
        @pl.when(pl.program_id(0) == 0)
        def _():
            def build(i, _):
                row = lax.broadcasted_iota(I32, (block, tokens), 0) + i * block
                hit = row == place_ref[0:1, :]
                for k in range(1, top):
                    hit = hit | (row == place_ref[k:k + 1, :])
                hot_ref[pl.ds(pl.multiple_of(i * block, block), block), :] = jnp.where(hit, 1.0, 0.0).astype(BF16)
                return 0

            lax.fori_loop(0, rows // block, build, 0)

        def step(i, _):
            at = pl.ds(pl.multiple_of(i * block, block), block)
            z_ref[at, :] = jnp.dot(hot_ref[at, :], x_ref[...], preferred_element_type=F32).astype(BF16)
            return 0

        lax.fori_loop(0, (used_ref[0] + block - 1) // block, step, 0)

    return pl.pallas_call(
        kernel,
        out_shape=jax.ShapeDtypeStruct((rows, d), BF16),
        grid_spec=pltpu.PrefetchScalarGridSpec(
            num_scalar_prefetch=1,
            grid=(d // tile,),
            in_specs=[
                pl.BlockSpec((top, tokens), lambda i, *_: (0, 0)),
                pl.BlockSpec((tokens, tile), lambda i, *_: (0, i)),
            ],
            out_specs=pl.BlockSpec((rows, tile), lambda i, *_: (0, i)),
            scratch_shapes=[pltpu.VMEM((rows, tokens), BF16)],
        ),
        compiler_params=params("arbitrary"),
        cost_estimate=pl.CostEstimate(flops=2 * rows * tokens * d, bytes_accessed=2 * (rows + tokens) * d, transcendentals=0),
        name="dispatch",
    )(rows_used, place, x)


def combine_matrix(place, gate, rows):
    sources, tokens, top = place.shape
    block = 128

    def kernel(place_ref, gate_ref, c_ref):
        column = lax.broadcasted_iota(I32, (block, rows), 1)
        total = jnp.zeros((block, rows), F32)
        for k in range(top):
            total = jnp.where(column == place_ref[0, :, k:k + 1], gate_ref[0, :, k:k + 1], total)
        c_ref[0] = total.astype(BF16)

    spec = pl.BlockSpec((1, block, top), lambda a, i: (a, i, 0))
    return pl.pallas_call(
        kernel,
        out_shape=jax.ShapeDtypeStruct((sources, tokens, rows), BF16),
        grid=(sources, tokens // block),
        in_specs=[spec, spec],
        out_specs=pl.BlockSpec((1, block, rows), lambda a, i: (a, i, 0)),
        compiler_params=params("arbitrary", "arbitrary"),
        cost_estimate=pl.CostEstimate(flops=sources * tokens * rows * top * 3, bytes_accessed=sources * tokens * rows * 2, transcendentals=0),
        name="combine_matrix",
    )(place, gate)


def up(count, source_at, expert_at, zs, w_gate, w_up, slots):
    experts, d, ff = w_gate.shape
    sources = len(zs)
    rows = sources * slots
    tile = 512
    sizes = list(range(64, rows + 1, 64))

    def kernel(count_ref, source_at_ref, expert_at_ref, *refs):
        z_refs, (wg_ref, wu_ref, h_ref, z_ref, sem) = refs[:sources], refs[sources:]
        e, f = pl.program_id(0), pl.program_id(1)

        def copies(e, act):
            slot = lax.rem(e, 2)
            for a in range(sources):
                for g in range(slots // GROUP):
                    @pl.when(g * GROUP < count_ref[a, e])
                    def _(a=a, g=g):
                        act(pltpu.make_async_copy(
                            z_refs[a].at[pl.ds(pl.multiple_of(source_at_ref[a, e] + g * GROUP, GROUP), GROUP), :],
                            z_ref.at[slot, pl.ds(pl.multiple_of(expert_at_ref[e, a] + g * GROUP, GROUP), GROUP), :],
                            sem.at[slot, a, g]))

        used = expert_at_ref[e, sources]

        @pl.when(f == 0)
        def _():
            @pl.when(e == 0)
            def _():
                copies(e, lambda c: c.start())

            copies(e, lambda c: c.wait())

            @pl.when(e + 1 < experts)
            def _():
                copies(e + 1, lambda c: c.start())

            z_ref[lax.rem(e, 2), pl.ds(pl.multiple_of(used, GROUP), 64), :] = jnp.zeros((64, d), BF16)

        for size in sizes:
            @pl.when((used > size - 64) & (used <= size))
            def _(size=size):
                z = z_ref[lax.rem(e, 2), :size, :]
                a = jnp.dot(z, wg_ref[0], preferred_element_type=F32)
                b = jnp.dot(z, wu_ref[0], preferred_element_type=F32)
                h_ref[0, :size, :] = (jax.nn.silu(a) * b).astype(BF16)

    weight = pl.BlockSpec((1, d, tile), lambda e, f, *_: (e, 0, f))
    return pl.pallas_call(
        kernel,
        out_shape=jax.ShapeDtypeStruct((experts, rows, ff), BF16),
        grid_spec=pltpu.PrefetchScalarGridSpec(
            num_scalar_prefetch=3,
            grid=(experts, ff // tile),
            in_specs=[ANY] * sources + [weight, weight],
            out_specs=pl.BlockSpec((1, rows, tile), lambda e, f, *_: (e, 0, f)),
            scratch_shapes=[
                pltpu.VMEM((2, rows + 64, d), BF16),
                pltpu.SemaphoreType.DMA((2, sources, slots // GROUP)),
            ],
        ),
        compiler_params=params("arbitrary", "arbitrary"),
        cost_estimate=pl.CostEstimate(
            flops=4 * experts * rows * d * ff, bytes_accessed=4 * experts * d * ff, transcendentals=experts * rows * ff),
        name="up",
    )(count, source_at, expert_at, *zs, w_gate, w_up)


def down(source_at, expert_at, h, w_down, c, first, width):
    experts, rows, ff = h.shape
    sources, tokens, columns = c.shape
    slots = rows // sources
    sizes = list(range(64, rows + 1, 64))
    depths = list(range(256, columns + 1, 256))
    tile = 256
    types = (F32, BF16, F32, BF16)

    def kernel(source_at_ref, expert_at_ref, h_ref, w_ref, c_ref, *refs):
        y_refs, (o_ref, out_ref) = refs[:sources], refs[sources:]
        e = pl.program_id(0)
        used = expert_at_ref[e, sources]

        @pl.when(e == 0)
        def _():
            o_ref[...] = jnp.zeros_like(o_ref)
            for a in range(sources):
                out_ref[a] = jnp.zeros(out_ref.shape[1:], BF16)

        for size in sizes:
            @pl.when((used > size - 64) & (used <= size))
            def _(size=size):
                o_ref[:size, :] = jnp.dot(h_ref[0, :size, :], w_ref[0], preferred_element_type=F32).astype(BF16)

        for a in range(sources):
            out_ref[a, pl.ds(pl.multiple_of(source_at_ref[a, e], GROUP), slots), :] = (
                o_ref[pl.ds(pl.multiple_of(expert_at_ref[e, a], GROUP), slots), :])

        @pl.when(e == experts - 1)
        def _():
            for a in range(sources):
                total = source_at_ref[a, experts]
                for depth in depths:
                    low = depth - 256 if depth > 256 else -1

                    @pl.when((total > low) & (total <= depth))
                    def _(a=a, depth=depth):
                        def part(i, _):
                            at = pl.ds(pl.multiple_of(i * tile, tile), tile)
                            y_refs[a][:, at] = jnp.dot(
                                c_ref[a, :, :depth], out_ref[a, :depth, at], preferred_element_type=F32).astype(types[a])
                            return 0

                        lax.fori_loop(0, width // tile, part, 0)

    step = first // width
    return pl.pallas_call(
        kernel,
        out_shape=[jax.ShapeDtypeStruct((tokens, width), t) for t in types],
        grid_spec=pltpu.PrefetchScalarGridSpec(
            num_scalar_prefetch=2,
            grid=(experts,),
            in_specs=[
                pl.BlockSpec((1, rows, ff), lambda e, *_: (e, 0, 0)),
                pl.BlockSpec((1, ff, width), lambda e, *_: (e, 0, step)),
                pl.BlockSpec((sources, tokens, columns), lambda e, *_: (0, 0, 0)),
            ],
            out_specs=[pl.BlockSpec((tokens, width), lambda e, *_: (0, 0))] * sources,
            scratch_shapes=[
                pltpu.VMEM((rows + slots, width), BF16),
                pltpu.VMEM((sources, columns + slots, width), BF16),
            ],
        ),
        compiler_params=params("arbitrary"),
        cost_estimate=pl.CostEstimate(
            flops=2 * experts * rows * ff * width, bytes_accessed=2 * experts * ff * width, transcendentals=0),
        name="down",
    )(source_at, expert_at, h, w_down, c)


def solution(mesh):
    members = mesh.shape["ep"]

    def swap(v, bit):
        return lax.ppermute(v, "ep", [(i, i ^ bit) for i in range(members)])

    def whole(x, expert, slot, gate, w_gate, w_up, w_down):
        tokens, top = expert.shape[2:]
        experts = w_gate.shape[0]
        slots = 5 * tokens * top // (4 * experts * members)
        rows = experts * slots
        x, expert, slot, gate = x[0, 0], expert[0, 0], slot[0, 0], gate[0, 0]

        routing = jnp.concatenate([
            expert.T.astype(F32), jnp.minimum(slot, slots).T.astype(F32), gate.T.astype(BF16).astype(F32)])
        near = swap(routing, 1)
        far = swap(routing, 2)
        across = swap(routing, 3)
        x1 = swap(x, 1)
        x2 = swap(x, 2)
        x3 = swap(x2, 1)

        routing = jnp.stack([routing, near, far, across])
        mine = routing[:, :top].astype(I32) - lax.axis_index("ep") * experts
        place = routing[:, top:2 * top].astype(I32)
        weight = routing[:, 2 * top:]
        kept = (mine >= 0) & (mine < experts) & (place < slots)
        mine = jnp.where(kept, mine, -1)
        is_at = mine[:, None] == jnp.arange(experts, dtype=I32)[None, :, None, None]
        count = jnp.max(jnp.where(is_at, place[:, None] + 1, 0), axis=(2, 3))
        size = (count + GROUP - 1) // GROUP * GROUP
        before = jnp.arange(experts + 1)[:, None] > jnp.arange(experts)[None, :]
        source_at = jnp.sum(jnp.where(before[None], size[:, None, :], 0), axis=2).astype(I32)
        before = jnp.arange(members + 1)[:, None] > jnp.arange(members)[None, :]
        expert_at = jnp.sum(jnp.where(before[None], size.T[:, None, :], 0), axis=2).astype(I32)
        shift = jnp.sum(jnp.where(is_at, source_at[:, :experts, None, None], 0), axis=1)
        place = jnp.where(kept, place + shift, -1)

        c = combine_matrix(place.swapaxes(1, 2), weight.swapaxes(1, 2), rows)
        zs = []
        for a, v in enumerate((x, x1, x2, x3)):
            zs.append(dispatch(source_at[a, experts:], place[a], v, rows))
        h = up(count, source_at, expert_at, zs, w_gate, w_up, slots)

        first, parts = 0, []
        for width in CHUNKS:
            own, near, far, across = down(source_at, expert_at, h, w_down, c, first, width)
            first += width
            met = (far + swap(across, 1).astype(F32)).astype(BF16)
            own = own + swap(near, 1).astype(F32)
            back = swap(met, 2)
            h, met = lax.optimization_barrier((h, met))
            parts.append((own, back))
        y = jnp.concatenate([(own + back.astype(F32)).astype(BF16) for own, back in parts], axis=1)
        return y[None, None]

    data, weights = P("dp", "ep"), P("ep")
    return jax.shard_map(
        whole, mesh=mesh, in_specs=(data,) * 4 + (weights,) * 3, out_specs=data, check_vma=False)
```

```python
import jax
import jax.numpy as jnp
from jax import lax
from jax.experimental import pallas as pl
from jax.experimental.pallas import tpu as pltpu
from jax.sharding import PartitionSpec as P

F32, BF16, I32 = jnp.float32, jnp.bfloat16, jnp.int32
VMEM_LIMIT = 64 * 1024 * 1024 - 64 * 1024 * 2
GROUP = 16
ANY = pl.BlockSpec(memory_space=pl.ANY)


def params(*semantics):
    return pltpu.CompilerParams(dimension_semantics=semantics, vmem_limit_bytes=VMEM_LIMIT)


def dispatch(rows_used, place, x, rows):
    top, tokens = place.shape
    d = x.shape[1]
    tile = min(d, 1024)
    block = 256

    def kernel(used_ref, place_ref, x_ref, z_ref, hot_ref):
        @pl.when(pl.program_id(0) == 0)
        def _():
            def build(i, _):
                row = lax.broadcasted_iota(I32, (block, tokens), 0) + i * block
                hit = row == place_ref[0:1, :]
                for k in range(1, top):
                    hit = hit | (row == place_ref[k:k + 1, :])
                hot_ref[pl.ds(pl.multiple_of(i * block, block), block), :] = jnp.where(hit, 1.0, 0.0).astype(BF16)
                return 0

            lax.fori_loop(0, rows // block, build, 0)

        def step(i, _):
            at = pl.ds(pl.multiple_of(i * block, block), block)
            z_ref[at, :] = jnp.dot(hot_ref[at, :], x_ref[...], preferred_element_type=F32).astype(BF16)
            return 0

        lax.fori_loop(0, (used_ref[0] + block - 1) // block, step, 0)

    return pl.pallas_call(
        kernel,
        out_shape=jax.ShapeDtypeStruct((rows, d), BF16),
        grid_spec=pltpu.PrefetchScalarGridSpec(
            num_scalar_prefetch=1,
            grid=(d // tile,),
            in_specs=[
                pl.BlockSpec((top, tokens), lambda i, *_: (0, 0)),
                pl.BlockSpec((tokens, tile), lambda i, *_: (0, i)),
            ],
            out_specs=pl.BlockSpec((rows, tile), lambda i, *_: (0, i)),
            scratch_shapes=[pltpu.VMEM((rows, tokens), BF16)],
        ),
        compiler_params=params("arbitrary"),
        cost_estimate=pl.CostEstimate(flops=2 * rows * tokens * d, bytes_accessed=2 * (rows + tokens) * d, transcendentals=0),
        name="dispatch",
    )(rows_used, place, x)


def combine_matrix(place, gate, rows):
    sources, tokens, top = place.shape
    block = 128

    def kernel(place_ref, gate_ref, c_ref):
        column = lax.broadcasted_iota(I32, (block, rows), 1)
        total = jnp.zeros((block, rows), F32)
        for k in range(top):
            total = jnp.where(column == place_ref[0, :, k:k + 1], gate_ref[0, :, k:k + 1], total)
        c_ref[0] = total.astype(BF16)

    spec = pl.BlockSpec((1, block, top), lambda a, i: (a, i, 0))
    return pl.pallas_call(
        kernel,
        out_shape=jax.ShapeDtypeStruct((sources, tokens, rows), BF16),
        grid=(sources, tokens // block),
        in_specs=[spec, spec],
        out_specs=pl.BlockSpec((1, block, rows), lambda a, i: (a, i, 0)),
        compiler_params=params("arbitrary", "arbitrary"),
        cost_estimate=pl.CostEstimate(flops=sources * tokens * rows * top * 3, bytes_accessed=sources * tokens * rows * 2, transcendentals=0),
        name="combine_matrix",
    )(place, gate)


def up(count, source_at, expert_at, zs, w_gate, w_up, slots):
    experts, d, ff = w_gate.shape
    sources = len(zs)
    rows = sources * slots
    tile = 512
    sizes = list(range(64, rows + 1, 64))

    def kernel(count_ref, source_at_ref, expert_at_ref, *refs):
        z_refs, (wg_ref, wu_ref, h_ref, z_ref, hs_ref, sem) = refs[:sources], refs[sources:]
        e, f = pl.program_id(0), pl.program_id(1)

        def copies(e, act):
            slot = lax.rem(e, 2)
            for a in range(sources):
                for g in range(slots // GROUP):
                    @pl.when(g * GROUP < count_ref[a, e])
                    def _(a=a, g=g):
                        act(pltpu.make_async_copy(
                            z_refs[a].at[pl.ds(pl.multiple_of(source_at_ref[a, e] + g * GROUP, GROUP), GROUP), :],
                            z_ref.at[slot, pl.ds(pl.multiple_of(expert_at_ref[e, a] + g * GROUP, GROUP), GROUP), :],
                            sem.at[slot, a, g]))

        used = expert_at_ref[e, sources]

        @pl.when(f == 0)
        def _():
            @pl.when(e == 0)
            def _():
                copies(e, lambda c: c.start())

            copies(e, lambda c: c.wait())

            @pl.when(e + 1 < experts)
            def _():
                copies(e + 1, lambda c: c.start())

            z_ref[lax.rem(e, 2), pl.ds(pl.multiple_of(used, GROUP), 64), :] = jnp.zeros((64, d), BF16)

        for size in sizes:
            @pl.when((used > size - 64) & (used <= size))
            def _(size=size):
                z = z_ref[lax.rem(e, 2), :size, :]
                a = jnp.dot(z, wg_ref[0], preferred_element_type=F32)
                b = jnp.dot(z, wu_ref[0], preferred_element_type=F32)
                hs_ref[:size, :] = (jax.nn.silu(a) * b).astype(BF16)

        hs_ref[pl.ds(pl.multiple_of(used, GROUP), slots), :] = jnp.zeros((slots, tile), BF16)
        for a in range(sources):
            h_ref[0, a * slots:(a + 1) * slots, :] = hs_ref[pl.ds(pl.multiple_of(expert_at_ref[e, a], GROUP), slots), :]

    weight = pl.BlockSpec((1, d, tile), lambda e, f, *_: (e, 0, f))
    return pl.pallas_call(
        kernel,
        out_shape=jax.ShapeDtypeStruct((experts, rows, ff), BF16),
        grid_spec=pltpu.PrefetchScalarGridSpec(
            num_scalar_prefetch=3,
            grid=(experts, ff // tile),
            in_specs=[ANY] * sources + [weight, weight],
            out_specs=pl.BlockSpec((1, rows, tile), lambda e, f, *_: (e, 0, f)),
            scratch_shapes=[
                pltpu.VMEM((2, rows + 64, d), BF16),
                pltpu.VMEM((rows + slots, tile), BF16),
                pltpu.SemaphoreType.DMA((2, sources, slots // GROUP)),
            ],
        ),
        compiler_params=params("arbitrary", "arbitrary"),
        cost_estimate=pl.CostEstimate(
            flops=4 * experts * rows * d * ff, bytes_accessed=4 * experts * d * ff, transcendentals=experts * rows * ff),
        name="up",
    )(count, source_at, expert_at, *zs, w_gate, w_up)


def finish(h, w_down, c):
    experts, rows, ff = h.shape
    sources, tokens, columns = c.shape
    d = w_down.shape[2]
    slots = rows // sources
    width, batch, lag = 512, 4, 2
    chunks, groups = d // width, experts // batch
    block = (tokens, width)

    def kernel(h_hbm, w_ref, c_hbm, y_hbm, h_ref, c_ref, out_ref, got3, got1, met, send3, send1, send2, far, own, y_ref,
               h_sem, c_sem, y_sem, send3_sem, send1_sem, send2_sem, got3_sem, got1_sem, met_sem):
        chunk, group = pl.program_id(0), pl.program_id(1)
        me = lax.axis_index("ep")
        beside = me + 1 - 2 * lax.rem(me, 2)
        across = lax.rem(me + 2, 4)
        half = lax.rem(chunk, 2)

        def load_h(g):
            at = pl.ds(pl.multiple_of(g * batch, batch), batch)
            return pltpu.make_async_copy(h_hbm.at[at], h_ref.at[at], h_sem.at[g])

        load_c = pltpu.make_async_copy(c_hbm, c_ref, c_sem)

        def remote(source, target, slot, sent, got, number, to):
            return pltpu.make_async_remote_copy(
                src_ref=source.at[slot], dst_ref=target.at[number], send_sem=sent.at[slot], recv_sem=got.at[number],
                device_id={"ep": to}, device_id_type=pl.DeviceIdType.MESH)

        def to_beside3(n):
            return remote(send3, got3, lax.rem(n, 2), send3_sem, got3_sem, n, beside)

        def to_beside1(n):
            return remote(send1, got1, lax.rem(n, 2), send1_sem, got1_sem, n, beside)

        def to_across(n):
            return remote(send2, met, lax.rem(n, 2), send2_sem, met_sem, n, across)

        def write(n):
            return pltpu.make_async_copy(
                y_ref.at[lax.rem(n, 2)], y_hbm.at[:, pl.ds(pl.multiple_of(n * width, width), width)], y_sem.at[lax.rem(n, 2)])

        @pl.when((chunk == 0) & (group == 0))
        def _():
            for g in range(groups):
                load_h(g).start()
            load_c.start()
            barrier = pltpu.get_barrier_semaphore()
            for to in (beside, across):
                pl.semaphore_signal(barrier, inc=1, device_id={"ep": to}, device_id_type=pl.DeviceIdType.MESH)
            pl.semaphore_wait(barrier, 2)

        @pl.when(chunk == 0)
        def _():
            load_h(group).wait()

        def expert(i, _):
            e = group * batch + i
            o = jnp.dot(h_ref[e], w_ref[i], preferred_element_type=F32).astype(BF16)
            for a in range(sources):
                out_ref[a, pl.ds(pl.multiple_of(e * slots, GROUP), slots), :] = o[a * slots:(a + 1) * slots]
            return 0

        lax.fori_loop(0, batch, expert, 0)

        @pl.when(group == groups - 1)
        def _():
            @pl.when(chunk == 0)
            def _():
                load_c.wait()

            @pl.when(chunk >= 2)
            def _():
                to_beside3(chunk - 2).wait_send()
                to_beside1(chunk - 2).wait_send()
                to_across(chunk - 2).wait_send()

            def share(a):
                return jnp.dot(c_ref[a], out_ref[a], preferred_element_type=F32)

            send3[half] = share(3).astype(BF16)
            send1[half] = share(1).astype(BF16)
            to_beside3(chunk).start()
            far[...] = share(2)
            to_beside1(chunk).start()
            own[lax.rem(chunk, lag + 1)] = share(0)
            to_beside3(chunk).wait_recv()
            send2[half] = (far[...] + got3[chunk].astype(F32)).astype(BF16)

            def close(n):
                to_beside1(n).wait_recv()
                to_across(n).wait_recv()

                @pl.when(n >= 2)
                def _():
                    write(n - 2).wait()

                y_ref[lax.rem(n, 2)] = (
                    own[lax.rem(n, lag + 1)] + got1[n].astype(F32) + met[n].astype(F32)).astype(BF16)
                write(n).start()

            to_across(chunk).start()

            @pl.when(chunk >= lag)
            def _():
                close(chunk - lag)

            @pl.when(chunk == chunks - 1)
            def _():
                for n in range(chunks - lag, chunks):
                    close(n)
                for n in range(chunks - 2, chunks):
                    to_beside3(n).wait_send()
                    to_beside1(n).wait_send()
                    to_across(n).wait_send()
                    write(n).wait()

    dma = pltpu.SemaphoreType.DMA
    return pl.pallas_call(
        kernel,
        out_shape=jax.ShapeDtypeStruct((tokens, d), BF16),
        grid=(chunks, groups),
        in_specs=[ANY, pl.BlockSpec((batch, ff, width), lambda n, g: (g, 0, n)), ANY],
        out_specs=ANY,
        scratch_shapes=[
            pltpu.VMEM((experts, rows, ff), BF16),
            pltpu.VMEM((sources, tokens, columns), BF16),
            pltpu.VMEM((sources, columns, width), BF16),
            pltpu.VMEM((chunks, *block), BF16),
            pltpu.VMEM((chunks, *block), BF16),
            pltpu.VMEM((chunks, *block), BF16),
            pltpu.VMEM((2, *block), BF16),
            pltpu.VMEM((2, *block), BF16),
            pltpu.VMEM((2, *block), BF16),
            pltpu.VMEM(block, F32),
            pltpu.VMEM((lag + 1, *block), F32),
            pltpu.VMEM((2, *block), BF16),
            dma((groups,)), dma, dma((2,)), dma((2,)), dma((2,)), dma((2,)), dma((chunks,)), dma((chunks,)), dma((chunks,)),
        ],
        compiler_params=pltpu.CompilerParams(
            dimension_semantics=("arbitrary", "arbitrary"), vmem_limit_bytes=VMEM_LIMIT, collective_id=0, has_side_effects=True),
        cost_estimate=pl.CostEstimate(
            flops=2 * experts * rows * ff * d, bytes_accessed=2 * experts * ff * d, transcendentals=0),
        name="finish",
    )(h, w_down, c)


def solution(mesh):
    members = mesh.shape["ep"]

    def swap(v, bit):
        return lax.ppermute(v, "ep", [(i, i ^ bit) for i in range(members)])

    def whole(x, expert, slot, gate, w_gate, w_up, w_down):
        tokens, top = expert.shape[2:]
        experts = w_gate.shape[0]
        slots = 5 * tokens * top // (4 * experts * members)
        rows = experts * slots
        x, expert, slot, gate = x[0, 0], expert[0, 0], slot[0, 0], gate[0, 0]

        routing = jnp.concatenate([
            expert.T.astype(F32), jnp.minimum(slot, slots).T.astype(F32), gate.T.astype(BF16).astype(F32)])
        near = swap(routing, 1)
        far = swap(routing, 2)
        across = swap(routing, 3)
        x1 = swap(x, 1)
        x2 = swap(x, 2)
        x3 = swap(x2, 1)

        routing = jnp.stack([routing, near, far, across])
        mine = routing[:, :top].astype(I32) - lax.axis_index("ep") * experts
        place = routing[:, top:2 * top].astype(I32)
        weight = routing[:, 2 * top:]
        kept = (mine >= 0) & (mine < experts) & (place < slots)
        mine = jnp.where(kept, mine, -1)
        is_at = mine[:, None] == jnp.arange(experts, dtype=I32)[None, :, None, None]
        count = jnp.max(jnp.where(is_at, place[:, None] + 1, 0), axis=(2, 3))
        size = (count + GROUP - 1) // GROUP * GROUP
        before = jnp.arange(experts + 1)[:, None] > jnp.arange(experts)[None, :]
        source_at = jnp.sum(jnp.where(before[None], size[:, None, :], 0), axis=2).astype(I32)
        before = jnp.arange(members + 1)[:, None] > jnp.arange(members)[None, :]
        expert_at = jnp.sum(jnp.where(before[None], size.T[:, None, :], 0), axis=2).astype(I32)
        shift = jnp.sum(jnp.where(is_at, source_at[:, :experts, None, None], 0), axis=1)
        fixed = jnp.where(kept, place + mine * slots, -1)
        place = jnp.where(kept, place + shift, -1)

        c = combine_matrix(fixed.swapaxes(1, 2), weight.swapaxes(1, 2), rows)
        zs = []
        for a, v in enumerate((x, x1, x2, x3)):
            zs.append(dispatch(source_at[a, experts:], place[a], v, rows))
        h = up(count, source_at, expert_at, zs, w_gate, w_up, slots)

        y = finish(h, w_down, c)
        return y[None, None]

    data, weights = P("dp", "ep"), P("ep")
    return jax.shard_map(
        whole, mesh=mesh, in_specs=(data,) * 4 + (weights,) * 3, out_specs=data, check_vma=False)
```

```python
import jax
import jax.numpy as jnp
from jax import lax
from jax.experimental import pallas as pl
from jax.experimental.pallas import tpu as pltpu
from jax.sharding import PartitionSpec as P

F32, BF16, I32 = jnp.float32, jnp.bfloat16, jnp.int32
VMEM_LIMIT = 64 * 1024 * 1024 - 64 * 1024 * 2
GROUP = 16
ANY = pl.BlockSpec(memory_space=pl.ANY)


def params(*semantics):
    return pltpu.CompilerParams(dimension_semantics=semantics, vmem_limit_bytes=VMEM_LIMIT)


def places(routes, experts, slots):
    sources = len(routes)
    top, tokens = routes[0].shape[0] // 3, routes[0].shape[1]

    def kernel(*refs):
        route_refs, (place_ref, pair_ref, count_ref, source_at_ref, expert_at_ref) = refs[:sources], refs[sources:]
        base = lax.axis_index("ep") * experts
        for a in range(sources):
            mine = route_refs[a][:top, :].astype(I32) - base
            slot = route_refs[a][top:2 * top, :].astype(I32)
            kept = (mine >= 0) & (mine < experts) & (slot < slots)
            mine = jnp.where(kept, mine, -1)
            gate = route_refs[a][2 * top:, :]
            here, place = jnp.int32(0), jnp.full((top, tokens), -1, I32)
            for e in range(experts):
                its = mine == e
                used = jnp.max(jnp.where(its, slot + 1, 0))
                count_ref[a, e] = used
                source_at_ref[a, e] = here
                place = jnp.where(its, slot + here, place)
                pair_ref[a, e:e + 1, :] = (jnp.max(jnp.where(its, slot + 1, 0), axis=0, keepdims=True) - 1).astype(F32)
                pair_ref[a, experts + e:experts + e + 1, :] = jnp.sum(jnp.where(its, gate, 0.0), axis=0, keepdims=True)
                here = here + (used + GROUP - 1) // GROUP * GROUP
            source_at_ref[a, experts] = here
            place_ref[a] = place
        for e in range(experts):
            here = jnp.int32(0)
            for a in range(sources):
                expert_at_ref[e, a] = here
                here = here + (count_ref[a, e] + GROUP - 1) // GROUP * GROUP
            expert_at_ref[e, sources] = here

    smem = pl.BlockSpec(memory_space=pltpu.SMEM)
    vmem = pl.BlockSpec(memory_space=pltpu.VMEM)
    return pl.pallas_call(
        kernel,
        out_shape=[
            jax.ShapeDtypeStruct((sources, top, tokens), I32),
            jax.ShapeDtypeStruct((sources, 2 * experts, tokens), F32),
            jax.ShapeDtypeStruct((sources, experts), I32),
            jax.ShapeDtypeStruct((sources, experts + 1), I32),
            jax.ShapeDtypeStruct((experts, sources + 1), I32),
        ],
        in_specs=[vmem] * sources,
        out_specs=[vmem, vmem, smem, smem, smem],
        cost_estimate=pl.CostEstimate(flops=1000000, bytes_accessed=400000, transcendentals=0),
        name="places",
    )(*routes)


def dispatch(rows_used, place, xs, rows):
    sources, top, tokens = place.shape
    width = xs[0].shape[1]
    block = 256
    tile = 1024

    def kernel(used_ref, place_ref, *refs):
        x_refs, z_ref = refs[:sources], refs[sources]
        i = pl.program_id(1)
        for a in range(sources):
            @pl.when((pl.program_id(0) == a) & (i * block < used_ref[a]))
            def _(a=a):
                row = lax.broadcasted_iota(I32, (block, tokens), 0) + i * block
                hit = row == place_ref[0, 0:1, :]
                for k in range(1, top):
                    hit = hit | (row == place_ref[0, k:k + 1, :])
                hot = jnp.where(hit, 1.0, 0.0).astype(BF16)
                for j in range(0, width, tile):
                    k = min(j + tile, width)
                    z_ref[0, :, j:k] = jnp.dot(hot, x_refs[a][:, j:k], preferred_element_type=F32).astype(BF16)

    return pl.pallas_call(
        kernel,
        out_shape=jax.ShapeDtypeStruct((sources, rows, width), BF16),
        grid_spec=pltpu.PrefetchScalarGridSpec(
            num_scalar_prefetch=1,
            grid=(sources, rows // block),
            in_specs=[pl.BlockSpec((1, top, tokens), lambda a, i, *_: (a, 0, 0))]
            + [pl.BlockSpec((tokens, width), lambda a, i, *_: (0, 0))] * sources,
            out_specs=pl.BlockSpec(
                (1, block, width),
                lambda a, i, used: (a, jnp.minimum(i, jnp.maximum(used[a] + block - 1, block) // block - 1), 0)),
        ),
        compiler_params=params("arbitrary", "arbitrary"),
        cost_estimate=pl.CostEstimate(
            flops=2 * sources * rows * tokens * width, bytes_accessed=4 * sources * rows * width, transcendentals=0),
        name="dispatch",
    )(rows_used, place, *xs)


def combine_matrix(pair, slots):
    sources, tokens, experts = pair.shape[0], pair.shape[1], pair.shape[2] // 2
    columns = experts * slots

    def kernel(pair_ref, c_ref):
        column = lax.broadcasted_iota(I32, (experts, columns), 1)
        own = lax.broadcasted_iota(I32, (experts, columns), 0)
        low = own * slots
        spread = jnp.where((column >= low) & (column < low + slots), 1.0, 0.0).astype(BF16)
        local = jnp.sum(jnp.where((column >= low) & (column < low + slots), column - low, 0), axis=0, keepdims=True).astype(F32)
        slot = jnp.dot(pair_ref[0, :, :experts].astype(BF16), spread, preferred_element_type=F32)
        gate = jnp.dot(pair_ref[0, :, experts:].astype(BF16), spread, preferred_element_type=F32)
        c_ref[0] = jnp.where(slot == local, gate, 0.0).astype(BF16)

    block = 256
    return pl.pallas_call(
        kernel,
        out_shape=jax.ShapeDtypeStruct((sources, tokens, columns), BF16),
        grid=(sources, tokens // block),
        in_specs=[pl.BlockSpec((1, block, 2 * experts), lambda a, i: (a, i, 0))],
        out_specs=pl.BlockSpec((1, block, columns), lambda a, i: (a, i, 0)),
        compiler_params=params("arbitrary", "arbitrary"),
        cost_estimate=pl.CostEstimate(flops=100000000, bytes_accessed=sources * tokens * columns * 2, transcendentals=0),
        name="combine_matrix",
    )(pair)


def up(first, depth, count, source_at, expert_at, z0, z2, z3, w_gate, w_up, slots, partial=None):
    experts, _, ff = w_gate.shape
    sources = count.shape[0]
    rows = sources * slots
    tile = 768 if depth <= 2048 else 512
    steps = ff // tile
    total = experts * steps
    unit = 64
    sizes = list(range(unit, rows + 1, unit))
    last = first > 0
    ahead, z_ahead, part_slots = 3, 2, 3

    def kernel(count_ref, source_at_ref, expert_at_ref, z0_ref, z2_ref, z3_ref, wg_hbm, wu_hbm, *refs):
        if last:
            partial_ref, h_ref, z_ref, part_ref, wg_ref, wu_ref, z_sem, part_sem, wg_sem, wu_sem, hs_ref = refs
        else:
            partial_ref, z_ref, part_ref, wg_ref, wu_ref, z_sem, part_sem, wg_sem, wu_sem = refs
        t = pl.program_id(0)
        e, f = t // steps, lax.rem(t, steps)
        now = lax.rem(t, part_slots)

        def start(c):
            c.start()

        def wait(c):
            c.wait()

        def weights(t, act):
            e, f, slot = t // steps, lax.rem(t, steps), lax.rem(t, ahead + 1)
            at = (e, pl.ds(first, depth), pl.ds(pl.multiple_of(f * tile, tile), tile))
            act(pltpu.make_async_copy(wg_hbm.at[at], wg_ref.at[slot], wg_sem.at[slot]))
            act(pltpu.make_async_copy(wu_hbm.at[at], wu_ref.at[slot], wu_sem.at[slot]))

        def inputs(e, act):
            slot = lax.rem(e, z_ahead + 1)
            for a in range(sources):
                source = (z0_ref.at[0], z0_ref.at[1], z2_ref.at[0], z3_ref.at[0])[a]
                columns = pl.ds(first if a < 2 else 0, depth)
                for g in range(slots // GROUP):
                    @pl.when(g * GROUP < count_ref[a, e])
                    def _(a=a, g=g, source=source, columns=columns):
                        act(pltpu.make_async_copy(
                            source.at[pl.ds(pl.multiple_of(source_at_ref[a, e] + g * GROUP, GROUP), GROUP), columns],
                            z_ref.at[slot, pl.ds(pl.multiple_of(expert_at_ref[e, a] + g * GROUP, GROUP), GROUP), :],
                            z_sem.at[slot, a, g]))

        def by_size(e, act):
            used = expert_at_ref[e, sources]
            for size in sizes:
                @pl.when((used > size - unit) & (used <= size))
                def _(size=size):
                    act(size)

        def sums(t, act):
            e, f, slot = t // steps, lax.rem(t, steps), lax.rem(t, part_slots)

            def one(size):
                here = part_ref.at[slot, :, pl.ds(0, size), :]
                there = partial_ref.at[e, :, pl.ds(0, size), pl.ds(pl.multiple_of(f * tile, tile), tile)]
                act(pltpu.make_async_copy(there, here, part_sem.at[slot]) if last
                    else pltpu.make_async_copy(here, there, part_sem.at[slot]))

            by_size(e, one)

        used = expert_at_ref[e, sources]

        @pl.when(t == 0)
        def _():
            for n in range(z_ahead):
                inputs(n, start)
            if last:
                for n in range(part_slots - 1):
                    sums(n, start)
            for n in range(ahead):
                weights(n, start)

        @pl.when(f == 0)
        def _():
            inputs(e, wait)

            @pl.when(e + z_ahead < experts)
            def _():
                inputs(e + z_ahead, start)

            z_ref[lax.rem(e, z_ahead + 1), pl.ds(pl.multiple_of(used, GROUP), unit), :] = jnp.zeros((unit, depth), BF16)

        if last:
            @pl.when(t + part_slots - 1 < total)
            def _():
                sums(t + part_slots - 1, start)

            sums(t, wait)
        else:
            @pl.when(t >= part_slots)
            def _():
                sums(t - part_slots, wait)

        @pl.when(t + ahead < total)
        def _():
            weights(t + ahead, start)

        weights(t, wait)

        def product(size):
            slot = lax.rem(t, ahead + 1)
            z = z_ref[lax.rem(e, z_ahead + 1), :size, :]
            a = jnp.dot(z, wg_ref[slot], preferred_element_type=F32)
            b = jnp.dot(z, wu_ref[slot], preferred_element_type=F32)
            if last:
                a, b = a + part_ref[now, 0, :size, :], b + part_ref[now, 1, :size, :]
                hs_ref[:size, :] = (jax.nn.silu(a) * b).astype(BF16)
            else:
                part_ref[now, 0, :size, :] = a
                part_ref[now, 1, :size, :] = b

        by_size(e, product)

        if last:
            hs_ref[pl.ds(pl.multiple_of(used, GROUP), slots), :] = jnp.zeros((slots, tile), BF16)
            for a in range(sources):
                h_ref[0, a * slots:(a + 1) * slots, :] = hs_ref[pl.ds(pl.multiple_of(expert_at_ref[e, a], GROUP), slots), :]
        else:
            sums(t, start)

            @pl.when(t == total - 1)
            def _():
                for n in range(total - part_slots, total):
                    sums(n, wait)

    dma = pltpu.SemaphoreType.DMA
    scratch = [
        pltpu.VMEM((z_ahead + 1, rows + unit, depth), BF16),
        pltpu.VMEM((part_slots, 2, rows, tile), F32),
        pltpu.VMEM((ahead + 1, depth, tile), BF16),
        pltpu.VMEM((ahead + 1, depth, tile), BF16),
        dma((z_ahead + 1, sources, slots // GROUP)),
        dma((part_slots,)),
        dma((ahead + 1,)),
        dma((ahead + 1,)),
    ]
    if last:
        out_shape = jax.ShapeDtypeStruct((experts, rows, ff), BF16)
        out_spec = pl.BlockSpec((1, rows, tile), lambda t, *_: (t // steps, 0, lax.rem(t, steps)))
        scratch.append(pltpu.VMEM((rows + slots, tile), BF16))
    else:
        out_shape, out_spec = jax.ShapeDtypeStruct((experts, 2, rows, ff), F32), ANY
    more = [partial] if last else []
    return pl.pallas_call(
        kernel,
        out_shape=out_shape,
        grid_spec=pltpu.PrefetchScalarGridSpec(
            num_scalar_prefetch=3,
            grid=(total,),
            in_specs=[ANY] * (5 + len(more)),
            out_specs=out_spec,
            scratch_shapes=scratch,
        ),
        compiler_params=params("arbitrary"),
        cost_estimate=pl.CostEstimate(
            flops=4 * experts * rows * depth * ff, bytes_accessed=4 * experts * depth * ff, transcendentals=0),
        name="up",
    )(count, source_at, expert_at, z0, z2, z3, w_gate, w_up, *more)


def finish(h, w_down, c):
    experts, rows, ff = h.shape
    sources, tokens, columns = c.shape
    d = w_down.shape[2]
    slots = rows // sources
    width, batch, lag = 512, 4, 2
    chunks, groups = d // width, experts // batch
    block = (tokens, width)

    def kernel(h_hbm, w_ref, c_hbm, y_hbm, h_ref, c_ref, out_ref, got3, got1, met, send3, send1, send2, far, own, y_ref,
               h_sem, c_sem, y_sem, send3_sem, send1_sem, send2_sem, got3_sem, got1_sem, met_sem):
        chunk, group = pl.program_id(0), pl.program_id(1)
        me = lax.axis_index("ep")
        beside = me + 1 - 2 * lax.rem(me, 2)
        across = lax.rem(me + 2, 4)
        half = lax.rem(chunk, 2)

        def load_h(g):
            at = pl.ds(pl.multiple_of(g * batch, batch), batch)
            return pltpu.make_async_copy(h_hbm.at[at], h_ref.at[at], h_sem.at[g])

        load_c = pltpu.make_async_copy(c_hbm, c_ref, c_sem)

        def remote(source, target, slot, sent, got, number, to):
            return pltpu.make_async_remote_copy(
                src_ref=source.at[slot], dst_ref=target.at[number], send_sem=sent.at[slot], recv_sem=got.at[number],
                device_id={"ep": to}, device_id_type=pl.DeviceIdType.MESH)

        def to_beside3(n):
            return remote(send3, got3, lax.rem(n, 2), send3_sem, got3_sem, n, beside)

        def to_beside1(n):
            return remote(send1, got1, lax.rem(n, 2), send1_sem, got1_sem, n, beside)

        def to_across(n):
            return remote(send2, met, lax.rem(n, 2), send2_sem, met_sem, n, across)

        def write(n):
            return pltpu.make_async_copy(
                y_ref.at[lax.rem(n, 2)], y_hbm.at[:, pl.ds(pl.multiple_of(n * width, width), width)], y_sem.at[lax.rem(n, 2)])

        @pl.when((chunk == 0) & (group == 0))
        def _():
            for g in range(groups):
                load_h(g).start()
            load_c.start()
            barrier = pltpu.get_barrier_semaphore()
            for to in (beside, across):
                pl.semaphore_signal(barrier, inc=1, device_id={"ep": to}, device_id_type=pl.DeviceIdType.MESH)
            pl.semaphore_wait(barrier, 2)

        @pl.when(chunk == 0)
        def _():
            load_h(group).wait()

        for i in range(batch):
            e = group * batch + i
            o = jnp.dot(h_ref[e], w_ref[i], preferred_element_type=F32).astype(BF16)
            for a in range(sources):
                out_ref[a, pl.ds(pl.multiple_of(e * slots, GROUP), slots), :] = o[a * slots:(a + 1) * slots]

        @pl.when(group == groups - 1)
        def _():
            @pl.when(chunk == 0)
            def _():
                load_c.wait()

            @pl.when(chunk >= 2)
            def _():
                to_beside3(chunk - 2).wait_send()
                to_beside1(chunk - 2).wait_send()
                to_across(chunk - 2).wait_send()

            def share(a):
                return jnp.dot(c_ref[a], out_ref[a], preferred_element_type=F32)

            send3[half] = share(3).astype(BF16)
            send1[half] = share(1).astype(BF16)
            to_beside3(chunk).start()
            far[...] = share(2)
            to_beside1(chunk).start()
            own[lax.rem(chunk, lag + 1)] = share(0)
            to_beside3(chunk).wait_recv()
            send2[half] = (far[...] + got3[chunk].astype(F32)).astype(BF16)

            def close(n):
                to_beside1(n).wait_recv()
                to_across(n).wait_recv()

                @pl.when(n >= 2)
                def _():
                    write(n - 2).wait()

                y_ref[lax.rem(n, 2)] = (
                    own[lax.rem(n, lag + 1)] + got1[n].astype(F32) + met[n].astype(F32)).astype(BF16)
                write(n).start()

            to_across(chunk).start()

            @pl.when(chunk >= lag)
            def _():
                close(chunk - lag)

            @pl.when(chunk == chunks - 1)
            def _():
                for n in range(chunks - lag, chunks):
                    close(n)
                for n in range(chunks - 2, chunks):
                    to_beside3(n).wait_send()
                    to_beside1(n).wait_send()
                    to_across(n).wait_send()
                    write(n).wait()

    dma = pltpu.SemaphoreType.DMA
    return pl.pallas_call(
        kernel,
        out_shape=jax.ShapeDtypeStruct((tokens, d), BF16),
        grid=(chunks, groups),
        in_specs=[ANY, pl.BlockSpec((batch, ff, width), lambda n, g: (g, 0, n)), ANY],
        out_specs=ANY,
        scratch_shapes=[
            pltpu.VMEM((experts, rows, ff), BF16),
            pltpu.VMEM((sources, tokens, columns), BF16),
            pltpu.VMEM((sources, columns, width), BF16),
            pltpu.VMEM((chunks, *block), BF16),
            pltpu.VMEM((chunks, *block), BF16),
            pltpu.VMEM((chunks, *block), BF16),
            pltpu.VMEM((2, *block), BF16),
            pltpu.VMEM((2, *block), BF16),
            pltpu.VMEM((2, *block), BF16),
            pltpu.VMEM(block, F32),
            pltpu.VMEM((lag + 1, *block), F32),
            pltpu.VMEM((2, *block), BF16),
            dma((groups,)), dma, dma((2,)), dma((2,)), dma((2,)), dma((2,)), dma((chunks,)), dma((chunks,)), dma((chunks,)),
        ],
        compiler_params=pltpu.CompilerParams(
            dimension_semantics=("arbitrary", "arbitrary"), vmem_limit_bytes=VMEM_LIMIT, collective_id=0, has_side_effects=True),
        cost_estimate=pl.CostEstimate(
            flops=2 * experts * rows * ff * d, bytes_accessed=2 * experts * ff * d, transcendentals=0),
        name="finish",
    )(h, w_down, c)


def solution(mesh):
    members = mesh.shape["ep"]

    def swap(v, bit):
        return lax.ppermute(v, "ep", [(i, i ^ bit) for i in range(members)])

    def whole(x, expert, slot, gate, w_gate, w_up, w_down):
        tokens, top = expert.shape[2:]
        experts = w_gate.shape[0]
        slots = 5 * tokens * top // (4 * experts * members)
        rows = experts * slots
        x, expert, slot, gate = x[0, 0], expert[0, 0], slot[0, 0], gate[0, 0]

        routing = jnp.concatenate([
            expert.T.astype(F32), jnp.minimum(slot, slots).T.astype(F32), gate.T.astype(BF16).astype(F32)])
        near = swap(routing, 1)
        far = swap(routing, 2)
        across = swap(routing, 3)
        x1 = swap(x, 1)
        middle = 3 * x.shape[1] // 8
        x2a = swap(x[:, :middle], 2)
        x3a = swap(x2a, 1)
        place, pair, count, source_at, expert_at = places((routing, near, far, across), experts, slots)
        used = source_at[:, experts:]
        counts, rest = [used[:2, 0], used[2], used[3]], x[:, middle:]
        put = [place[:2], place[2:3], place[3:]]
        counts, put, pair, xb = lax.optimization_barrier((counts, put, pair.swapaxes(1, 2), rest))
        x2b = swap(xb, 2)
        x3b = swap(x2b, 1)
        z0 = dispatch(counts[0], put[0], (x, x1), rows)
        c = combine_matrix(pair, slots)
        z2 = dispatch(counts[1], put[1], (x2a,), rows)
        z3 = dispatch(counts[2], put[2], (x3a,), rows)
        partial = up(0, middle, count, source_at, expert_at, z0, z2, z3, w_gate, w_up, slots)
        z2 = dispatch(counts[1], put[1], (x2b,), rows)
        z3 = dispatch(counts[2], put[2], (x3b,), rows)
        h = up(middle, x.shape[1] - middle, count, source_at, expert_at, z0, z2, z3, w_gate, w_up, slots, partial=partial)
        y = finish(h, w_down, c)
        return y[None, None]

    data, weights = P("dp", "ep"), P("ep")
    return jax.shard_map(
        whole, mesh=mesh, in_specs=(data,) * 4 + (weights,) * 3, out_specs=data, check_vma=False)
```
